32 devices in a mesh: section: 2 (over core), seq: 16 (over z, y, x).
Axes of the slice: x: 2, y: 2, z: 4, core: 2. Of those that a mesh axis runs over, the one named last changes fastest.
Arguments:
- acts: bfloat16 [2, 4096, 2048], P('section', 'seq'), may hold values from -6 to 6
- in_proj: bfloat16 [2, 2048, 4640], P('section', 'seq'), may hold values from -0.125 to 0.125
- out_proj: bfloat16 [2, 2048, 2048], P('section'), may hold values from -0.125 to 0.125
- conv_weight: float32 [2, 4, 2304], P('section'), may hold values from -3 to 3
- conv_bias: float32 [2, 2304], P('section'), may hold values from -3 to 3
- dt_bias: float32 [2, 32], P('section'), may hold values from -4 to -1
- decay_rate: float32 [2, 32], P('section'), may hold values from 0.0001 to 0.5
- skip_gain: float32 [2, 32], P('section'), may hold values from -4 to 4
- level_bias: float32 [2, 256], P('section'), may hold values from -4 to 4
- norm_gain: float32 [2, 2048], P('section'), may hold values from 0.5 to 1.5
- gate_gain: float32 [2, 2048], P('section'), may hold values from 0.5 to 1.5
Outputs:
- handoff: bfloat16 [2, 4096, 2048], P('section', 'seq')
The draws below stay inside these ranges and needn't reach their ends.
All inputs are finite; a program needn't handle non-finite values.
Results may differ from the reference program's by a relative error of at most 0.006.
Values may be sent and summed in bfloat16 or wider, within the bound.
A program may use at most 128 MiB of HBM per device.

```python
import math
import jax
import jax.numpy as jnp
from jax import lax

D = 2048
CONV = 4
HEADS = 32
LEVELS = 8
SECTIONS = 2
DI = 2048
CH = 2304
PROJ = 4640
SEQLEN = 4096
N_SEQ = 16


def block_levels(key, extent, shards, low, largest):
    loudness = 1.0
    for axis_at, parts in shards:
        steps = jax.random.uniform(jax.random.fold_in(jax.random.fold_in(key, 6), axis_at), (parts,), jnp.float32, low / len(shards), largest / len(shards))
        loudness = loudness * jnp.repeat(jnp.exp(steps), extent[axis_at] // parts).reshape((-1,) + (1,) * (len(extent) - 1 - axis_at))
    return loudness


def normal_values(key, extent, width, reach, pieces=(), kind=jnp.bfloat16):
    loudness = block_levels(key, extent, pieces, -0.22, 0.18) if pieces else 1.0
    values = jax.random.normal(key, extent, jnp.float32) * width * loudness
    return jnp.minimum(jnp.maximum(values, -reach), reach).astype(kind)


def setup_inputs(seed: int = 0) -> dict:
    streams_of = jax.random.split(jax.random.key(seed), 12)
    acts = normal_values(streams_of[0], (SECTIONS, SEQLEN, D), 1.0, 6.0, ((0, 2), (1, 16)))
    in_proj = normal_values(streams_of[1], (SECTIONS, D, PROJ), D ** -0.5, 0.125, ((0, 2), (1, 16)))
    out_proj = normal_values(streams_of[2], (SECTIONS, DI, D), DI ** -0.5, 0.125, ((0, 2),))
    conv_weight = normal_values(streams_of[3], (SECTIONS, CONV, CH), 0.6, 3.0, ((0, 2),), jnp.float32)
    conv_bias = normal_values(streams_of[4], (SECTIONS, CH), 0.5, 3.0, ((0, 2),), jnp.float32)
    dt_bias = jnp.clip(-4.0 + 3.0 * jax.random.uniform(streams_of[5], (SECTIONS, HEADS), jnp.float32) ** block_levels(streams_of[5], (SECTIONS, HEADS), ((0, 2),), -0.2, 0.2), -4.0, -1.0)
    decay_rate = jnp.clip(jnp.exp(math.log(0.5) - 8.517193 * jax.random.uniform(streams_of[6], (SECTIONS, HEADS), jnp.float32) ** block_levels(streams_of[6], (SECTIONS, HEADS), ((0, 2),), -0.2, 0.2)), 0.0001, 0.5)
    skip_gain = normal_values(streams_of[7], (SECTIONS, HEADS), 1.0, 4.0, ((0, 2),), jnp.float32)
    level_bias = normal_values(streams_of[8], (SECTIONS, HEADS * LEVELS), 1.0, 4.0, ((0, 2),), jnp.float32)
    norm_gain = jnp.clip(1.0 + 0.1 * jax.random.normal(streams_of[9], (SECTIONS, D), jnp.float32), 0.5, 1.5)
    gate_gain = jnp.clip(1.0 + 0.1 * jax.random.normal(streams_of[10], (SECTIONS, DI), jnp.float32), 0.5, 1.5)
    return dict(acts=acts, in_proj=in_proj, out_proj=out_proj, conv_weight=conv_weight, conv_bias=conv_bias, dt_bias=dt_bias, decay_rate=decay_rate, skip_gain=skip_gain, level_bias=level_bias, norm_gain=norm_gain, gate_gain=gate_gain)


EPS = 1e-05
best_precision = lax.Precision.HIGHEST

def block_core(operands):
    c_block, b_block, x_block, cum_block, dt_block, lam_block = operands
    length = c_block.shape[0]
    scores = jnp.dot(c_block, b_block.T, precision=best_precision, preferred_element_type=jnp.float32)
    row_ids = lax.broadcasted_iota(jnp.int32, (length, length), 0)
    col_ids = lax.broadcasted_iota(jnp.int32, (length, length), 1)
    causal = (col_ids <= row_ids)[:, :, None]
    differ = cum_block[:, None, :] - cum_block[None, :, :]
    decays = jnp.where(causal, jnp.exp(jnp.where(causal, differ, 0.0)), 0.0)
    weights = decays * scores[:, :, None] * dt_block[None, :, :] * lam_block[:, None, :]
    y_block = jnp.einsum('tsh,shp->thp', weights, x_block, precision=best_precision)
    tail = jnp.exp(cum_block[-1][None, :] - cum_block) * dt_block
    state = jnp.einsum('sn,shp->hnp', b_block, x_block * tail[:, :, None], precision=best_precision)
    return (y_block, state)

def mixer(acts, w_in, w_out, conv_w, conv_b, dt_b, rate, skip, lam_b, gain_in, gain_gate):
    hidden = acts.astype(jnp.float32)
    seqlen = hidden.shape[0]
    inner = gain_gate.shape[0]
    heads = dt_b.shape[0]
    head_size = inner // heads
    chans = conv_w.shape[1]
    state_size = (chans - inner) // 2
    kernel_len = conv_w.shape[0]
    normed_in = (hidden * lax.rsqrt(lax.optimization_barrier(jnp.mean(hidden * hidden, axis=1, keepdims=True)) + EPS) * gain_in).astype(jnp.bfloat16)
    projected = jnp.dot(normed_in, w_in, preferred_element_type=jnp.float32).astype(jnp.bfloat16)
    conv_in = jnp.concatenate([jnp.zeros((kernel_len - 1, chans), jnp.float32), projected[:, :chans].astype(jnp.float32)], axis=0)
    mixed = conv_b + jnp.zeros((seqlen, chans), jnp.float32)
    for offset in range(kernel_len):
        mixed = mixed + conv_w[offset] * conv_in[offset:offset + seqlen]
    mixed = jax.nn.silu(mixed)
    values = mixed[:, :inner].reshape(seqlen, heads, head_size)
    b_mat = mixed[:, inner:inner + state_size]
    c_mat = mixed[:, inner + state_size:]
    z_gate = projected[:, chans:chans + inner].astype(jnp.float32)
    steps = jax.nn.softplus(projected[:, chans + inner:chans + inner + heads].astype(jnp.float32) + dt_b)
    lam = jax.nn.softplus(projected[:, chans + inner + heads:].astype(jnp.float32) + lam_b).reshape(seqlen, heads, LEVELS)
    blocks = N_SEQ
    length = seqlen // blocks
    log_decay = (-steps * rate).reshape(blocks, length, heads)
    cum = jnp.cumsum(log_decay, axis=1)
    x_blocks = values.reshape(blocks, length, heads, head_size)
    b_blocks = b_mat.reshape(blocks, length, state_size)
    c_blocks = c_mat.reshape(blocks, length, state_size)
    dt_blocks = steps.reshape(blocks, length, heads)
    lam_blocks = lam.reshape(blocks, length, heads, LEVELS)
    y_all, states = lax.map(block_core, (c_blocks, b_blocks, x_blocks, cum, dt_blocks, lam_blocks[..., 0]))
    y_all = y_all + skip[None, None, :, None] * x_blocks
    endlog = cum[:, -1, :]
    inclusive = jnp.cumsum(endlog, axis=0)
    exclusive = inclusive - endlog
    for level in range(1, blocks.bit_length()):
        half = 2 ** (level - 1)
        groups = blocks // (2 * half)
        lower_states = states.reshape(groups, 2, half, heads, state_size, head_size)[:, 0]
        incl_groups = inclusive.reshape(groups, 2, half, heads)
        lower_end = incl_groups[:, 0, half - 1]
        weights = jnp.exp(lower_end[:, None, :] - incl_groups[:, 0])
        summed = jnp.einsum('gjh,gjhnp->ghnp', weights, lower_states, precision=best_precision)
        upper_excl = exclusive.reshape(groups, 2, half, heads)[:, 1]
        carry = jnp.exp(upper_excl - lower_end[:, None, :])
        c_upper = c_blocks.reshape(groups, 2, half, length, state_size)[:, 1]
        reads = jnp.einsum('gitn,ghnp->githp', c_upper, summed, precision=best_precision)
        cum_upper = cum.reshape(groups, 2, half, length, heads)[:, 1]
        lam_upper = lam_blocks.reshape(groups, 2, half, length, heads, LEVELS)[:, 1, :, :, :, level]
        scale = carry[:, :, None, :] * jnp.exp(cum_upper) * lam_upper
        shaped = y_all.reshape(groups, 2, half, length, heads, head_size)
        y_all = shaped.at[:, 1].add(reads * scale[..., None]).reshape(blocks, length, heads, head_size)
    y_flat = y_all.reshape(seqlen, inner)
    gated = y_flat * jax.nn.silu(z_gate)
    normed = (gated * lax.rsqrt(lax.optimization_barrier(jnp.mean(gated * gated, axis=1, keepdims=True)) + EPS) * gain_gate).astype(jnp.bfloat16)
    return (hidden + jnp.dot(normed, w_out, preferred_element_type=jnp.float32)).astype(jnp.bfloat16)

def reference(acts, in_proj, out_proj, conv_weight, conv_bias, dt_bias, decay_rate, skip_gain, level_bias, norm_gain, gate_gain):
    results = []
    for section_id in range(SECTIONS):
        results.append(mixer(acts[section_id], in_proj[section_id], out_proj[section_id], conv_weight[section_id], conv_bias[section_id], dt_bias[section_id], decay_rate[section_id], skip_gain[section_id], level_bias[section_id], norm_gain[section_id], gate_gain[section_id]))
    stacked = jnp.stack(results, axis=0)
    return jnp.roll(stacked, 1, axis=0)
```

```python
import functools

import jax
import jax.numpy as jnp
from jax import lax
from jax.experimental import pallas as pl
from jax.experimental.pallas import tpu as pltpu
from jax.sharding import PartitionSpec as P

EPS = 1e-05
MESH = pl.DeviceIdType.MESH
f32 = jnp.float32
bf16 = jnp.bfloat16
HIGHEST = lax.Precision.HIGHEST


def remote(src, dst, send, recv, seq, axis="seq"):
    return pltpu.make_async_remote_copy(
        src_ref=src,
        dst_ref=dst,
        send_sem=send,
        recv_sem=recv,
        device_id={axis: seq},
        device_id_type=MESH,
    )


def greet(seq, axis="seq"):
    pl.semaphore_signal(
        pltpu.get_barrier_semaphore(), inc=1, device_id={axis: seq}, device_id_type=MESH
    )


def partner(inner, step, group):
    low = lax.rem(lax.rem(inner, 2) + step % 2, 2)
    high = lax.rem(inner // 2 + step // 2, max(group // 2, 1))
    return high * 2 + low


def selector(lanes, wide, size, first, stride):
    row = lax.broadcasted_iota(jnp.int32, (lanes, wide), 0)
    head = lax.broadcasted_iota(jnp.int32, (lanes, wide), 1) // size
    return jnp.where(row == head * stride + first, 1.0, 0.0).astype(bf16)


def spread(value, pick):
    high = value.astype(bf16)
    low = (value - high.astype(f32)).astype(bf16)
    return jnp.dot(high, pick, preferred_element_type=f32) + jnp.dot(
        low, pick, preferred_element_type=f32
    )


def silu(value):
    return value / (1.0 + jnp.exp(-value))


def softplus(value):
    return jnp.maximum(value, 0.0) + jnp.log1p(jnp.exp(-jnp.abs(value)))


def layer_kernel(
    dims, group, n, levels, used, sections,
    acts_ref, w_hbm, wo_hbm, taps_ref, cbias_ref, small_bias_ref, rate_ref, skip_ref,
    norm_ref, gate_ref, out_ref,
    u_all, w_own, tail_v, w_a, w_z, w_o, p_a, halo, before_s, picks, x_s, bc_s, small_s, cum_s,
    st, bucket, whole_st, xs_own, xs_got, xl_own, xl_got, y_s, q_own, q_got, o_acc, o_v,
    load_sem, u_send, u_recv, w_send, up_send, down_send, w_recv,
    bc_up, bc_down, bc_peer, bc_recv, zg_send, zg_recv, zu_send, zd_send, z_recv,
    halo_sem, xs_sem, xl_sem, q_send, q_recv, ho_send, ho_recv,
):
    wide, state, size, taps, z_from, lanes = dims
    section = lax.axis_index("section")
    me = lax.axis_index("seq")
    outer = me // group
    inner = lax.rem(me, group)
    outers = n // group
    base = outer * group
    length = acts_ref.shape[0]
    rows = w_hbm.shape[0]
    depth = group * rows
    chunks, _, _, cw = w_z.shape
    hs = wide // size
    main = wide + lanes
    columns = main + 2 * state
    bc_from = group * wide
    bits = group.bit_length() - 1
    keep = halo.shape[0]
    has_up = outer < outers - 1
    has_down = outer > 0
    p1 = partner(inner, 1, group)
    p2 = partner(inner, 2, group)
    p3 = partner(inner, 3, group)

    def at_rows(slot):
        return pl.ds(pl.multiple_of(slot * rows, rows), rows)

    def slot_at(source, slot, lo, hi):
        return w_a.at[source, at_rows(slot), lo:hi]

    def main_slot(source, slot):
        return slot_at(source, slot, 0, main)

    def bc_slot(source, slot):
        return slot_at(source, slot, main, columns)

    def x_cols(peer):
        return pl.ds(pl.multiple_of(peer * wide, wide), wide)

    def z_cols(peer, c):
        return pl.ds(pl.multiple_of(z_from + peer * wide + c * cw, 128), cw)

    load_all = pltpu.make_async_copy(w_hbm, w_own, load_sem.at[0])
    load_all.start()
    load_x = pltpu.make_async_copy(
        w_hbm.at[:, x_cols(inner)], slot_at(outer, inner, 0, wide), load_sem.at[1]
    )
    load_x.start()
    load_bc = pltpu.make_async_copy(
        w_hbm.at[:, bc_from : bc_from + 2 * state], bc_slot(outer, inner), load_sem.at[2]
    )
    load_bc.start()

    count = group - 1 + has_up.astype(jnp.int32) + has_down.astype(jnp.int32) + 1
    for step in range(1, group):
        greet(base + partner(inner, step, group))

    @pl.when(has_up)
    def _():
        greet(me + group)

    @pl.when(has_down)
    def _():
        greet(me - group)

    def twin(bit):
        half = 1 << bit
        return me + half - 2 * half * lax.rem(me // half, 2)

    for bit in range(bits, used):
        greet(twin(bit))
    greet(lax.rem(section + sections - 1, sections), "section")
    pl.semaphore_wait(pltpu.get_barrier_semaphore(), count + used - bits)

    def up(source, slot):
        at = source * group + slot
        piece = main_slot(source, slot)
        return remote(piece, piece, up_send.at[at], w_recv.at[at], me + group)

    def down(source, slot):
        at = source * group + slot
        piece = main_slot(source, slot)
        return remote(piece, piece, down_send.at[at], w_recv.at[at], me - group)

    def along(source, step):
        piece = bc_slot(source, inner)
        here = bc_recv.at[source * group + inner]
        if step > 0:
            return remote(piece, piece, bc_up.at[source], here, me + group)
        return remote(piece, piece, bc_down.at[source], here, me - group)

    def across(source, step):
        piece = bc_slot(source, inner)
        peer = base + partner(inner, step, group)
        at = source * group
        return remote(piece, piece, bc_peer.at[at + step], bc_recv.at[at + inner], peer)

    def arrived(source, slot):
        piece = main_slot(source, slot)
        remote(piece, piece, w_send.at[0], w_recv.at[source * group + slot], me).wait_recv()

    def bc_arrived(source, slot):
        piece = bc_slot(source, slot)
        remote(piece, piece, w_send.at[0], bc_recv.at[source * group + slot], me).wait_recv()

    def give_x(step):
        peer = partner(inner, step, group)
        remote(
            w_own.at[:, x_cols(peer)], slot_at(outer, inner, 0, wide),
            w_send.at[step], w_recv.at[me], base + peer,
        ).start()

    def give_tail(step):
        peer = partner(inner, step, group)
        remote(
            tail_v.at[peer], slot_at(outer, inner, wide, main),
            w_send.at[step], w_recv.at[me], base + peer,
        ).start()

    def give_z(step):
        peer = partner(inner, step, group)
        for c in range(chunks):
            remote(
                w_own.at[:, z_cols(peer, c)], w_z.at[c, outer, at_rows(inner)],
                zg_send.at[step], zg_recv.at[inner], base + peer,
            ).start()

    load_all.wait()
    for step in range(1, group):
        give_x(step)
    load_bc.wait()

    @pl.when(has_up)
    def _():
        along(outer, 1).start()

    @pl.when(has_down)
    def _():
        along(outer, -1).start()

    tail_from = z_from + group * wide
    tail = w_own.shape[1] - tail_from
    row = lax.broadcasted_iota(jnp.int32, (tail, lanes), 0)
    col = lax.broadcasted_iota(jnp.int32, (tail, lanes), 1)
    narrow = w_own[:, tail_from:]
    for peer in range(group):
        steps_at = peer * hs + col
        levels_at = group * hs + peer * hs * levels + col - hs
        source = jnp.where(col < hs, steps_at, levels_at)
        source = jnp.where(col < hs + hs * levels, source, -1)
        pick = jnp.where(row == source, 1.0, 0.0).astype(bf16)
        tail_v[peer] = jnp.dot(narrow, pick, preferred_element_type=f32).astype(bf16)
    w_a[outer, at_rows(inner), wide:main] = tail_v[inner]
    load_x.wait()
    for step in range(1, group):
        give_tail(step)

    @pl.when(has_up)
    def _():
        up(outer, inner).start()

    @pl.when(has_down)
    def _():
        down(outer, inner).start()

    piece_rows = 32

    def norm(step, carry):
        at = pl.ds(pl.multiple_of(step * piece_rows, piece_rows), piece_rows)
        value = acts_ref[at].astype(f32)
        scale = lax.rsqrt(jnp.mean(value * value, axis=1, keepdims=True) + EPS)
        u_all[inner, at] = (value * scale * norm_ref[...]).astype(bf16)
        return carry

    lax.fori_loop(0, length // piece_rows, norm, 0)

    for step in range(1, group):
        slot = partner(inner, step, group)
        arrived(outer, slot)

        @pl.when(has_up)
        def _():
            up(outer, slot).start()

        @pl.when(has_down)
        def _():
            down(outer, slot).start()

    half_rows = length // 2

    def u_half(block, h):
        return u_all.at[block, h * half_rows : (h + 1) * half_rows]

    def u_copy(block, h, at, peer):
        piece = u_half(block, h)
        return remote(piece, piece, u_send.at[at], u_recv.at[block * 2 + h], base + peer)

    u_sends = [
        u_copy(inner, 1, 0, p1),
        u_copy(inner, 0, 1, p2),
        u_copy(inner, 0, 2, p1),
        u_copy(inner, 1, 3, p2),
    ]
    u_relays = [u_copy(p1, 1, 4, p2), u_copy(p2, 0, 5, p1)]

    def u_arrived(block, h):
        piece = u_half(block, h)
        remote(piece, piece, u_send.at[0], u_recv.at[block * 2 + h], me).wait_recv()

    for copy in u_sends:
        copy.start()
    for step in range(1, group):
        across(outer, step).start()

    for c in range(chunks):
        pltpu.make_async_copy(
            w_hbm.at[:, z_cols(inner, c)], w_z.at[c, outer, at_rows(inner)], load_sem.at[3]
        ).start()
    z_own = w_z.at[:, outer, at_rows(inner)]
    for c in range(chunks):
        for j in range(group):
            pltpu.make_async_copy(
                wo_hbm.at[j * wide + c * cw : j * wide + (c + 1) * cw],
                w_o.at[c, j * cw : (j + 1) * cw],
                load_sem.at[4],
            ).start()
    for step in range(1, group):
        give_z(step)
    picks[0] = selector(lanes, wide, size, 0, 1)

    def fill(level, carry):
        picks[level + 1] = selector(lanes, wide, size, hs + level, levels)
        return carry

    lax.fori_loop(0, used + 1, fill, 0)

    @pl.when(jnp.logical_not(has_down))
    def _():
        halo[...] = jnp.zeros(halo.shape, halo.dtype)

    def relay(distance, block):
        slot = partner(inner, block, group)

        @pl.when(outer - distance >= 0)
        def _():
            source = outer - distance
            arrived(source, slot)

            @pl.when(has_up)
            def _():
                up(source, slot).start()

            @pl.when(block == 0)
            def _():
                bc_arrived(source, inner)

                @pl.when(has_up)
                def _():
                    along(source, 1).start()

                for step in range(1, group):
                    across(source, step).start()

        @pl.when(outer + distance < outers)
        def _():
            source = outer + distance
            arrived(source, slot)

            @pl.when(has_down)
            def _():
                down(source, slot).start()

            @pl.when(block == 0)
            def _():
                bc_arrived(source, inner)

                @pl.when(has_down)
                def _():
                    along(source, -1).start()

                for step in range(1, group):
                    across(source, step).start()

    def relay_step(step, carry):
        relay(step // group, lax.rem(step, group))
        return carry

    def up_z(source, c):
        at = c * outers + source
        piece = w_z.at[c, source]
        return remote(piece, piece, zu_send.at[at], z_recv.at[at], me + group)

    def down_z(source, c):
        at = c * outers + source
        piece = w_z.at[c, source]
        return remote(piece, piece, zd_send.at[at], z_recv.at[at], me - group)

    def z_arrived(source, c):
        piece = w_z.at[c, source]
        remote(piece, piece, zu_send.at[0], z_recv.at[c * outers + source], me).wait_recv()

    def own_z(c):
        @pl.when(has_up)
        def _():
            up_z(outer, c).start()

        @pl.when(has_down)
        def _():
            down_z(outer, c).start()

    def service(c):
        def step_of(distance, carry):
            @pl.when(jnp.logical_and(outer - distance >= 0, has_up))
            def _():
                z_arrived(outer - distance, c)
                up_z(outer - distance, c).start()

            @pl.when(jnp.logical_and(outer + distance < outers, has_down))
            def _():
                z_arrived(outer + distance, c)
                down_z(outer + distance, c).start()

            return carry

        lax.fori_loop(1, outers - 1, step_of, 0)

    def settle(c):
        def step_of(distance, carry):
            @pl.when(jnp.logical_and(outer - distance >= 0, jnp.logical_not(has_up)))
            def _():
                z_arrived(outer - distance, c)

            @pl.when(jnp.logical_and(outer + distance < outers, jnp.logical_not(has_down)))
            def _():
                z_arrived(outer + distance, c)

            return carry

        lax.fori_loop(1, outers, step_of, 0)

    lax.fori_loop(group, min(2, outers) * group, relay_step, 0)
    u_arrived(p1, 1)
    u_relays[0].start()
    u_arrived(p2, 0)
    u_relays[1].start()
    if outers > 2:
        lax.fori_loop(2 * group, (outers - 1) * group, relay_step, 0)
    pltpu.make_async_copy(z_own, z_own, load_sem.at[3]).wait()
    for step in range(1, group):
        slot = partner(inner, step, group)
        piece = w_z.at[:, outer, at_rows(slot)]
        remote(piece, piece, zg_send.at[0], zg_recv.at[slot], me).wait_recv()
    own_z(0)
    own_z(1)
    if outers > 2:
        lax.fori_loop((outers - 1) * group, outers * group, relay_step, 0)
    own_z(2)
    service(0)
    u_arrived(p1, 0)
    u_arrived(p2, 1)

    def ready(source, carry):
        for step in range(1, group):
            bc_arrived(source, partner(inner, step, group))
        return carry

    lax.fori_loop(0, outers, ready, 0)

    def multiply(step, carry):
        block = partner(inner, step, group)
        every = w_a[...].reshape(outers * depth, columns)
        part = jnp.dot(u_all[block], every, preferred_element_type=f32)
        p_a[block] = part.astype(bf16)
        return carry

    lax.fori_loop(0, group - 1, multiply, 0)
    own_z(3)
    service(1)
    u_arrived(p3, 0)
    u_arrived(p3, 1)
    multiply(group - 1, 0)
    edge = remote(
        p_a.at[group - 1, length - keep :], halo, halo_sem.at[0], halo_sem.at[1], me + group
    )

    @pl.when(has_up)
    def _():
        edge.start()

    taps_x = taps_ref.at[:, x_cols(inner)]
    mine = jnp.concatenate([taps_x[...], taps_ref[:, bc_from:]], axis=1)
    mine_bias = jnp.concatenate(
        [cbias_ref[:, x_cols(inner)], cbias_ref[:, bc_from:]], axis=1
    )

    def state_work(step, carry):
        block = lax.rem(step + 1, group)

        @pl.when(jnp.logical_and(step == group - 1, has_down))
        def _():
            edge.wait_recv()

        @pl.when(block == 0)
        def _():
            before_s[...] = halo[...]

        @pl.when(block > 0)
        def _():
            before_s[...] = p_a[jnp.maximum(block - 1, 0), length - keep :]

        raw = jnp.concatenate([p_a[block, :, :wide], p_a[block, :, main:]], axis=1).astype(f32)
        last = before_s[...].astype(f32)
        last = jnp.concatenate([last[:, :wide], last[:, main:]], axis=1)
        ext = jnp.concatenate([last, raw], axis=0)
        first = keep - taps + 1
        mixed = mine_bias + mine[taps - 1 :] * raw
        for k in range(taps - 1):
            mixed = mixed + mine[k : k + 1] * ext[first + k : first + k + length]
        mixed = silu(mixed)
        x = mixed[:, :wide]
        x_s[block] = x.astype(bf16)
        bc = mixed[:, wide:].astype(bf16)
        bc_s[block] = bc
        small = softplus(p_a[block, :, wide:main].astype(f32) + small_bias_ref[inner])
        small_s[block] = small
        rows_at = lax.broadcasted_iota(jnp.int32, (length, length), 0)
        cols_at = lax.broadcasted_iota(jnp.int32, (length, length), 1)
        below = jnp.where(cols_at <= rows_at, 1.0, 0.0)
        cum = jnp.dot(
            below, -small * rate_ref[inner], precision=HIGHEST, preferred_element_type=f32
        )
        cum_s[block] = cum
        fade = jnp.exp(cum[length - 1 :] - cum) * small
        faded = (x * spread(fade, picks[0])).astype(bf16)
        st[block] = lax.dot_general(
            bc[:, :state], faded, (((0,), (0,)), ((), ())), preferred_element_type=f32
        )
        return carry

    lax.fori_loop(0, group, state_work, 0)
    service(2)

    def widened(log):
        value = jnp.broadcast_to(jnp.exp(log), (8, lanes))
        return jnp.dot(
            value, picks[0].astype(f32), precision=HIGHEST, preferred_element_type=f32
        )[:1]

    ends = [cum_s[b, length - 1 :] for b in range(group)]
    part_rows = 32
    logs = list(ends)
    before = [jnp.zeros_like(ends[0]) for _ in range(group)]
    plan = []
    for bit in range(bits):
        half = 1 << bit
        joins, uppers, next_logs = [], [], []
        for g in range(len(logs) // 2):
            for b in range(2 * g * half + half, 2 * (g + 1) * half):
                uppers.append((b, g, None if bit == 0 else widened(before[b])))
                before[b] = before[b] + logs[2 * g]
            joins.append(widened(logs[2 * g + 1]))
            next_logs.append(logs[2 * g] + logs[2 * g + 1])
        plan.append((joins, uppers))
        logs = next_logs
    block_log = logs[0]
    before_log = jnp.zeros_like(block_log)

    def local_join(step, carry):
        at = pl.ds(pl.multiple_of(step * part_rows, part_rows), part_rows)
        summed = [st[b, at] for b in range(group)]
        for bit, (joins, uppers) in enumerate(plan):
            taken = set()
            for b, g, factor in uppers:
                value = summed[2 * g]
                if factor is not None:
                    value = factor * value
                bucket[b, bit, at] = value.astype(bf16)
                taken.add(b)
            for b in range(group):
                if b not in taken:
                    bucket[b, bit, at] = jnp.zeros((part_rows, wide), bf16)
            summed = [
                factor * summed[2 * g] + summed[2 * g + 1] for g, factor in enumerate(joins)
            ]
        whole_st[at] = summed[0]
        if used > bits:
            xs_own[0, at] = summed[0].astype(bf16)
        return carry

    lax.fori_loop(0, state // part_rows, local_join, 0)

    def swap(k):
        peer = twin(bits + k)
        return (
            remote(xl_own.at[k], xl_got.at[k], xl_sem.at[2 * k], xl_sem.at[2 * k + 1], peer),
            remote(xs_own.at[k], xs_got.at[k], xs_sem.at[2 * k], xs_sem.at[2 * k + 1], peer),
        )

    def send_state(k):
        xl_own[k] = jnp.broadcast_to(block_log, (8, lanes))
        for copy in swap(k):
            copy.start()

    if used > bits:
        send_state(0)

    def inside(block, carry):
        bc = bc_s[block]
        scores = lax.dot_general(
            bc[:, state:], bc[:, :state], (((1,), (1,)), ((), ())), preferred_element_type=f32
        )
        rows_at = lax.broadcasted_iota(jnp.int32, (length, length), 0)
        cols_at = lax.broadcasted_iota(jnp.int32, (length, length), 1)
        causal = cols_at <= rows_at
        small = small_s[block]
        cum = cum_s[block]
        cum_rows = jnp.transpose(cum)
        x = x_s[block].astype(f32)
        stepped = (x * spread(small, picks[0])).astype(bf16)
        parts = []
        for h in range(hs):
            differ = cum[:, h : h + 1] - cum_rows[h : h + 1, :]
            weights = jnp.exp(jnp.where(causal, differ, -1e30)) * scores
            parts.append(
                jnp.dot(
                    weights.astype(bf16),
                    stepped[:, h * size : (h + 1) * size],
                    preferred_element_type=f32,
                )
            )
        y = jnp.concatenate(parts, axis=1)
        y_s[block] = y * spread(small, picks[1]) + skip_ref[inner] * x
        return carry

    lax.fori_loop(0, group, inside, 0)
    service(3)

    def reads(lo, hi):
        def work(block, carry):
            c = bc_s[block, :, state:]
            small = small_s[block]
            total = None
            for level in range(lo, hi):
                value = jnp.dot(c, bucket[block, level], preferred_element_type=f32)
                term = value * spread(small, picks[level + 2])
                total = term if total is None else total + term
            y_s[block] += total * spread(jnp.exp(cum_s[block]), picks[0])
            return carry

        lax.fori_loop(0, group, work, 0)

    done = 0
    for k in range(used - bits):
        if k > 0 and k == used - bits - 1:
            reads(done, bits + k)
            done = bits + k
        for copy in swap(k):
            copy.wait_recv()
        other_log = xl_got[k][:1]
        upper = lax.rem(me // (1 << (bits + k)), 2)
        is_upper = jnp.broadcast_to(upper, (1, wide)) == 1
        lane_upper = jnp.broadcast_to(upper, (1, lanes)) == 1
        factors = [
            jnp.where(is_upper, widened(before_log + before[b]), 0.0) for b in range(group)
        ]
        mine_by = jnp.where(is_upper, 1.0, widened(other_log))
        other_by = jnp.where(is_upper, widened(block_log), 1.0)
        more = k + 1 < used - bits

        def join(step, carry):
            at = pl.ds(pl.multiple_of(step * part_rows, part_rows), part_rows)
            other = xs_got[k, at].astype(f32)
            for b in range(group):
                bucket[b, bits + k, at] = (factors[b] * other).astype(bf16)
            if more:
                total = other_by * other + mine_by * whole_st[at]
                whole_st[at] = total
                xs_own[k + 1, at] = total.astype(bf16)
            return carry

        lax.fori_loop(0, state // part_rows, join, 0)
        before_log = jnp.where(lane_upper, before_log + other_log, before_log)
        block_log = block_log + other_log
        if more:
            send_state(k + 1)
    reads(done, used)

    def copy_to(c, step):
        peer = partner(inner, group - step, group)
        return remote(
            q_own.at[c, peer], q_got.at[c, inner],
            q_send.at[c * group + step], q_recv.at[c * group + inner], base + peer,
        )

    def gate(c, block):
        every = w_z[c].reshape(outers * depth, cw)
        z = jnp.dot(u_all[block], every, preferred_element_type=f32)
        z = z.astype(bf16).astype(f32)
        y = y_s[block, :, pl.ds(pl.multiple_of(c * cw, cw), cw)]
        return (y * silu(z)).astype(bf16)

    def gate_all(c):
        settle(c)

        def work(step, carry):
            block = partner(inner, group - step, group)
            q_own[c, block] = gate(c, block)

            @pl.when(step > 1)
            def _():
                copy_to(c, step - 1).start()

            return carry

        lax.fori_loop(1, group, work, 0)
        q_got[c, inner] = gate(c, inner)
        copy_to(c, group - 1).start()

    def collect(c):
        for step in range(1, group):
            peer = partner(inner, step, group)
            piece = q_got.at[c, peer]
            remote(
                piece, piece, q_send.at[0], q_recv.at[c * group + peer], me
            ).wait_recv()

    def joined(c, at):
        q = jnp.concatenate([q_got[c, j, at] for j in range(group)], axis=1).astype(f32)
        squares = jnp.sum(q * q, axis=1, keepdims=True)
        return (q * gate_ref[c]).astype(bf16), squares

    everything = pl.ds(0, length)
    gate_all(0)
    pltpu.make_async_copy(w_o, w_o, load_sem.at[4]).wait()
    o_acc[...] = jnp.zeros(o_acc.shape, f32)

    def rounds(c, squares):
        gate_all(c)
        collect(c - 1)
        q, more = joined(c - 1, everything)
        o_acc[...] += jnp.dot(q, w_o[c - 1], preferred_element_type=f32)
        return squares + more

    squares = lax.fori_loop(1, chunks, rounds, jnp.zeros((length, 1), f32))
    collect(chunks - 1)
    parts = 2
    part = length // parts
    following = lax.rem(section + 1, sections)
    handoffs = []
    for r in range(parts):
        at = pl.ds(r * part, part)
        q, more = joined(chunks - 1, at)
        total = o_acc[at] + jnp.dot(q, w_o[chunks - 1], preferred_element_type=f32)
        mean = (squares[r * part : (r + 1) * part] + more) / (wide * group)
        o_v[at] = (acts_ref[at].astype(f32) + total * lax.rsqrt(mean + EPS)).astype(bf16)
        copy = remote(
            o_v.at[at], out_ref.at[at], ho_send.at[r], ho_recv.at[r], following, "section"
        )
        handoffs.append(copy)
        if r > 0:
            handoffs[r - 1].start()
    handoffs[-1].start()

    def drain(at, carry):
        source = at // group
        slot = lax.rem(at, group)

        @pl.when(jnp.logical_and(has_up, source <= outer))
        def _():
            up(source, slot).wait_send()

            @pl.when(slot == 0)
            def _():
                along(source, 1).wait_send()

        @pl.when(jnp.logical_and(has_down, source >= outer))
        def _():
            down(source, slot).wait_send()

            @pl.when(slot == 0)
            def _():
                along(source, -1).wait_send()

        @pl.when(slot == 0)
        def _():
            for step in range(1, group):
                across(source, step).wait_send()

        return carry

    lax.fori_loop(0, n, drain, 0)

    def drain_z(at, carry):
        c = at // outers
        source = lax.rem(at, outers)

        @pl.when(jnp.logical_and(has_up, source <= outer))
        def _():
            up_z(source, c).wait_send()

        @pl.when(jnp.logical_and(has_down, source >= outer))
        def _():
            down_z(source, c).wait_send()

        return carry

    lax.fori_loop(0, chunks * outers, drain_z, 0)
    for step in range(1, group):
        piece = main_slot(outer, inner)
        remote(piece, piece, w_send.at[step], w_recv.at[me], me).wait_send()
        remote(z_own, z_own, zg_send.at[step], zg_recv.at[inner], me).wait_send()
        for c in range(chunks):
            copy_to(c, step).wait_send()
    for copy in u_sends + u_relays:
        copy.wait_send()

    @pl.when(has_up)
    def _():
        edge.wait_send()

    for k in range(used - bits):
        for copy in swap(k):
            copy.wait_send()
    for copy in handoffs:
        copy.wait()


def layer(dims, group, n, levels, used, sections, chunks, args):
    wide, state, size, taps, z_from, lanes = dims
    acts, w = args[0], args[1]
    length, width = acts.shape
    rows = w.shape[0]
    outers = n // group
    columns = wide + lanes + 2 * state
    cw = wide // chunks
    bits = group.bit_length() - 1
    swaps = max(used - bits, 1)
    dma = pltpu.SemaphoreType.DMA
    vmem = pl.BlockSpec(memory_space=pltpu.VMEM)
    anywhere = pl.BlockSpec(memory_space=pl.ANY)
    return pl.pallas_call(
        functools.partial(layer_kernel, dims, group, n, levels, used, sections),
        out_shape=jax.ShapeDtypeStruct((length, width), bf16),
        in_specs=[vmem, anywhere, anywhere] + [vmem] * (len(args) - 3),
        out_specs=vmem,
        scratch_shapes=[
            pltpu.VMEM((group, length, width), bf16),
            pltpu.VMEM(w.shape, bf16),
            pltpu.VMEM((group, rows, lanes), bf16),
            pltpu.VMEM((outers, group * rows, columns), bf16),
            pltpu.VMEM((chunks, outers, group * rows, cw), bf16),
            pltpu.VMEM((chunks, group * cw, width), bf16),
            pltpu.VMEM((group, length, columns), bf16),
            pltpu.VMEM((16, columns), bf16),
            pltpu.VMEM((16, columns), bf16),
            pltpu.VMEM((used + 2, lanes, wide), bf16),
            pltpu.VMEM((group, length, wide), bf16),
            pltpu.VMEM((group, length, 2 * state), bf16),
            pltpu.VMEM((group, length, lanes), f32),
            pltpu.VMEM((group, length, lanes), f32),
            pltpu.VMEM((group, state, wide), f32),
            pltpu.VMEM((group, used, state, wide), bf16),
            pltpu.VMEM((state, wide), f32),
            pltpu.VMEM((swaps, state, wide), bf16),
            pltpu.VMEM((swaps, state, wide), bf16),
            pltpu.VMEM((swaps, 8, lanes), f32),
            pltpu.VMEM((swaps, 8, lanes), f32),
            pltpu.VMEM((group, length, wide), f32),
            pltpu.VMEM((chunks, group, length, cw), bf16),
            pltpu.VMEM((chunks, group, length, cw), bf16),
            pltpu.VMEM((length, width), f32),
            pltpu.VMEM((length, width), bf16),
            dma((5,)),
            dma((6,)),
            dma((2 * group,)),
            dma((group,)),
            dma((n,)),
            dma((n,)),
            dma((n,)),
            dma((outers,)),
            dma((outers,)),
            dma((n,)),
            dma((n,)),
            dma((group,)),
            dma((group,)),
            dma((chunks * outers,)),
            dma((chunks * outers,)),
            dma((chunks * outers,)),
            dma((2,)),
            dma((2 * swaps,)),
            dma((2 * swaps,)),
            dma((chunks * group,)),
            dma((chunks * group,)),
            dma((2,)),
            dma((2,)),
        ],
        compiler_params=pltpu.CompilerParams(
            collective_id=0, has_side_effects=True, vmem_limit_bytes=60 << 20
        ),
    )(*args)


def per_device(
    acts,
    in_proj,
    out_proj,
    conv_weight,
    conv_bias,
    dt_bias,
    decay_rate,
    skip_gain,
    level_bias,
    norm_gain,
    gate_gain,
):
    n = lax.axis_size("seq")
    sections = lax.axis_size("section")
    group = min(4, n)
    inner = gate_gain.shape[1]
    heads = dt_bias.shape[1]
    head_size = inner // heads
    chans = conv_weight.shape[2]
    state = (chans - inner) // 2
    taps = conv_weight.shape[1]
    levels = level_bias.shape[1] // heads
    used = n.bit_length() - 1
    wide = inner // group
    hs = heads // group
    tail = hs + hs * levels
    lanes = -(-tail // 128) * 128
    chunks = wide // 128

    small_bias = jnp.concatenate(
        [dt_bias.reshape(group, 1, hs), level_bias.reshape(group, 1, hs * levels)], axis=2
    )
    small_bias = jnp.pad(small_bias, ((0, 0), (0, 0), (0, lanes - tail)))
    rate = jnp.pad(decay_rate.reshape(group, 1, hs), ((0, 0), (0, 0), (0, lanes - hs)))
    skip = jnp.repeat(skip_gain[0], head_size).reshape(group, 1, wide)
    gate = jnp.swapaxes(gate_gain.reshape(group, chunks, wide // chunks), 0, 1)
    gate = gate.reshape(chunks, 1, group * (wide // chunks))
    result = layer(
        (wide, state, head_size, taps, chans, lanes),
        group,
        n,
        levels,
        used,
        sections,
        chunks,
        (
            acts[0],
            in_proj[0],
            out_proj[0],
            conv_weight[0],
            conv_bias,
            small_bias,
            rate,
            skip,
            norm_gain,
            gate,
        ),
    )
    return result[None]


def solution(mesh):
    return jax.shard_map(
        per_device,
        mesh=mesh,
        in_specs=(
            P("section", "seq", None),
            P("section", "seq", None),
            P("section", None, None),
            P("section", None, None),
            P("section", None),
            P("section", None),
            P("section", None),
            P("section", None),
            P("section", None),
            P("section", None),
            P("section", None),
        ),
        out_specs=P("section", "seq", None),
        check_vma=False,
    )
```
